256 devices in a mesh: gx: 16 (over z, core), gy: 4 (over y), gz: 4 (over x).
Axes of the slice: x: 4, y: 4, z: 8, core: 2. Of those that a mesh axis runs over, the one named last changes fastest.
Arguments:
- images: bfloat16 [256, 5, 524288], P(('gx', 'gy', 'gz')), may hold values from 0 to 0.015625
- order: int32 [256], replicated, may hold values from 0 to 255, as said below
Outputs:
- frame: float32 [5, 524288], P(None, 'gx')
The draws below stay inside these ranges and needn't reach their ends.
Inputs may be any that keep to these rules, and one draw needn't show every extreme that they name: order is a permutation of the bricks, where brick r sits at index r // 16 along gx, (r // 4) % 4 along gy and r % 4 along gz; the bricks of one gz index take consecutive places, within them the bricks of one (gy, gz) pair take consecutive places; the order of gz indices, the order of gy indices within each gz index and the order of gx indices within each (gy, gz) pair are arbitrary and may differ from slab to slab and from column to column.
All inputs are finite; a program needn't handle non-finite values.
Results may differ from the reference program's by a relative error of at most 0.0003.
Values may be sent and summed in bfloat16 or wider, within the bound.
No kernel may reach another device: no remote copies, remote signals or barrier semaphores. Data moves between devices by JAX's collectives and lax.ppermute only.
A program may use at most 64 MiB of HBM per device.

```python
import jax
import jax.numpy as jnp
from jax import lax

CHANNELS = 5
RANKS = 256
PIXELS = 524288
N_GX = 16
N_GY = 4
N_GZ = 4


def random_places(key, shape, count):
    scores = jax.random.randint(key, shape + (count,), 0, 1 << 20, dtype=jnp.int32)
    scores = scores * count + jnp.arange(count, dtype=jnp.int32)
    ranked = jnp.argsort(scores, axis=-1)
    return jnp.argsort(ranked, axis=-1).astype(jnp.int32)


def draw_order(key, part):
    place_z = random_places(jax.random.fold_in(key, 11), (), N_GZ)
    place_y = random_places(jax.random.fold_in(key, 13), (N_GZ,), N_GY)
    place_x = random_places(jax.random.fold_in(key, 17), (N_GY, N_GZ), N_GX)
    slab = place_z[None, None, :]
    column = jnp.transpose(place_y, (1, 0))[None, :, :]
    within = jnp.transpose(place_x, (2, 0, 1))
    grid = slab * (N_GY * N_GX) + column * N_GX + within
    return grid.reshape(-1).astype(jnp.int32)


def levels(own_key, extent, split, least, largest):
    gain = 1.0
    for axis_at, shards_of in split:
        steps = jax.random.uniform(jax.random.fold_in(jax.random.fold_in(own_key, 6), axis_at), (shards_of,), jnp.float32, least / len(split), largest / len(split))
        gain = gain * jnp.repeat(jnp.exp(steps), extent[axis_at] // shards_of).reshape((-1,) + (1,) * (len(extent) - 1 - axis_at))
    return gain


def setup_inputs(seed: int = 0) -> dict:
    keys = jax.random.split(jax.random.key(seed), 3)
    return {
        "images": jnp.clip(0.015625 * jax.random.uniform(keys[0], (RANKS, CHANNELS, PIXELS), jnp.float32) ** levels(keys[0], (RANKS, CHANNELS, PIXELS), ((0, 256),), -0.2, 0.2), 0.0, 0.015625).astype(jnp.bfloat16),
        "order": draw_order(jax.random.fold_in(keys[2], 71), 0),
    }


def reference(images, order):
    places = jnp.arange(RANKS, dtype=jnp.int32)
    brick = jnp.zeros((RANKS,), jnp.int32).at[order.astype(jnp.int32)].set(places)

    def layer(total, member):
        picture = lax.dynamic_index_in_dim(images, member, 0, keepdims=False).astype(jnp.float32)
        return total + (1.0 - total[4:5]) * picture, None

    start = jnp.zeros((images.shape[1], images.shape[2]), jnp.float32)
    total, _ = lax.scan(layer, start, brick)
    return total
```

```python
import jax
import jax.numpy as jnp
from jax import lax
from jax.experimental import pallas as pl
from jax.experimental.pallas import tpu as pltpu
from jax.sharding import PartitionSpec as P


DEPTH_RANGE = 4.02
STEPS = 65535.0 / DEPTH_RANGE


def opacity_kernel(images, out):
    rows, lanes = out.shape[1:]
    for p in range(out.shape[0]):
        out[p] = images[0, images.shape[1] - 1, p * rows * lanes : (p + 1) * rows * lanes].reshape(rows, lanes)


def opacity_tiles(images, count, rows, lanes):
    step = 64
    return pl.pallas_call(
        opacity_kernel,
        grid=(count // step,),
        in_specs=[pl.BlockSpec((1, images.shape[1], step * rows * lanes), lambda i: (0, 0, i))],
        out_specs=pl.BlockSpec((step, rows, lanes), lambda i: (i, 0, 0)),
        out_shape=jax.ShapeDtypeStruct((count, rows, lanes), images.dtype),
        compiler_params=pltpu.CompilerParams(vmem_limit_bytes=16 << 20),
        cost_estimate=pl.CostEstimate(flops=images.size, bytes_accessed=2 * images.size, transcendentals=0),
        name="opacity_tiles",
    )(images)


def front_kernel(brick, opacity, codes, total):
    count = opacity.shape[0]

    def place(p, done):
        r = brick[p]
        left = 1.0 - done
        code = jnp.floor(jnp.log(left) * -STEPS + 0.5).astype(jnp.int32) - 32768
        codes[r] = code.astype(jnp.int16)
        return done + left * opacity[r].astype(jnp.float32)

    total[...] = lax.fori_loop(0, count, place, jnp.zeros(total.shape, jnp.float32), unroll=8)


def front(brick, opacity):
    count, rows, lanes = opacity.shape
    return pl.pallas_call(
        front_kernel,
        in_specs=[
            pl.BlockSpec(memory_space=pltpu.SMEM),
            pl.BlockSpec(memory_space=pltpu.VMEM),
        ],
        out_specs=[
            pl.BlockSpec(memory_space=pltpu.VMEM),
            pl.BlockSpec(memory_space=pltpu.VMEM),
        ],
        out_shape=[
            jax.ShapeDtypeStruct((count, rows, lanes), jnp.int16),
            jax.ShapeDtypeStruct((rows, lanes), jnp.float32),
        ],
        cost_estimate=pl.CostEstimate(flops=8 * opacity.size, bytes_accessed=4 * opacity.size, transcendentals=opacity.size),
        compiler_params=pltpu.CompilerParams(vmem_limit_bytes=16 << 20),
        name="front",
    )(brick, opacity)


def blend_kernel(member, codes, *refs):
    pictures, out = refs[:-1], refs[-1]
    for g in range(out.shape[0]):
        sums = [jnp.zeros(out.shape[2:], jnp.float32) for _ in range(out.shape[1])]
        for j, picture in enumerate(pictures):
            code = codes[g, member[j]].astype(jnp.int32).astype(jnp.float32)
            left = jnp.exp((code + 32768.0) * (-1.0 / STEPS))
            for c in range(out.shape[1]):
                sums[c] = sums[c] + left * picture[c, g].astype(jnp.float32)
        for c in range(out.shape[1]):
            out[g, c] = sums[c]


def blend(member, codes, pictures, step=4):
    bands, members, rows, lanes = codes.shape
    colours = pictures[0].shape[0]
    return pl.pallas_call(
        blend_kernel,
        grid_spec=pltpu.PrefetchScalarGridSpec(
            num_scalar_prefetch=1,
            grid=(bands // step,),
            in_specs=[pl.BlockSpec((step, members, rows, lanes), lambda i, m: (i, 0, 0, 0))]
            + [pl.BlockSpec((colours, step, rows, lanes), lambda i, m: (0, i, 0, 0)) for _ in pictures],
            out_specs=pl.BlockSpec((step, colours, rows, lanes), lambda i, m: (i, 0, 0, 0)),
        ),
        out_shape=jax.ShapeDtypeStruct((bands, colours, rows, lanes), jnp.float32),
        cost_estimate=pl.CostEstimate(
            flops=2 * colours * codes.size, bytes_accessed=2 * (colours + 1) * codes.size, transcendentals=codes.size
        ),
        compiler_params=pltpu.CompilerParams(vmem_limit_bytes=24 << 20),
        name="blend",
    )(member, codes, *pictures)


def per_device(images, order):
    count_x = lax.axis_size("gx")
    count_y = lax.axis_size("gy")
    count_z = lax.axis_size("gz")
    plane = count_y * count_z
    bricks = count_x * plane
    channels, pixels = images.shape[1:]
    colours = channels - 1
    lanes = 128
    rows = pixels // (bricks * lanes)
    place_y = lax.axis_index("gy")
    place_z = lax.axis_index("gz")

    opacity = opacity_tiles(images, bricks, rows, lanes)
    opacity = lax.all_to_all(opacity, ("gx", "gy", "gz"), 0, 0, tiled=True)

    places = jnp.arange(bricks, dtype=jnp.int32)
    brick = jnp.sum(jnp.where(order[None, :] == places[:, None], places[None, :], 0), axis=1, dtype=jnp.int32)

    colour_tiles = images[0, :colours].reshape(colours, count_x, plane, rows, lanes)
    pictures, member = [], []
    for dy in range(count_y):
        for dz in range(count_z):
            target = ((place_y + dy) % count_y) * count_z + (place_z + dz) % count_z
            piece = lax.dynamic_index_in_dim(colour_tiles, target, 2, keepdims=False)
            if dy or dz:
                moves = [
                    (a * count_z + b, ((a + dy) % count_y) * count_z + (b + dz) % count_z)
                    for a in range(count_y)
                    for b in range(count_z)
                ]
                piece = lax.ppermute(piece, ("gy", "gz"), moves)
            pictures.append(piece)
            member.append(((place_y - dy) % count_y) * count_z + (place_z - dz) % count_z)
    member = jnp.stack(member).astype(jnp.int32)

    codes, total = front(brick, opacity)
    codes = lax.all_to_all(codes, "gx", 0, 0, tiled=True).reshape(count_x, plane, rows, lanes)
    part = blend(member, codes, pictures)
    part = lax.all_to_all(part, "gx", 0, 0, tiled=True)
    piece = jnp.concatenate([jnp.sum(part, axis=0), total[None]], axis=0)
    piece = piece.reshape(channels, 1, rows * lanes)
    band = lax.all_to_all(jnp.broadcast_to(piece, (channels, plane, rows * lanes)), ("gy", "gz"), 1, 1, tiled=True)
    return band.reshape(channels, -1)


def solution(mesh):
    in_specs = (P(("gx", "gy", "gz"), None, None), P())
    out_specs = P(None, "gx")

    return jax.shard_map(per_device, mesh=mesh, in_specs=in_specs, out_specs=out_specs, check_vma=False)
```
